32 devices in a mesh: grp: 8 (over z, y), mem: 4 (over x, core).
Axes of the slice: x: 2, y: 2, z: 4, core: 2. Of those that a mesh axis runs over, the one named last changes fastest.
Arguments:
- client_input: bfloat16 [8, 4, 128, 896], P('grp', 'mem'), may hold values from -6 to 6
- client_gain: float32 [4, 896], P('mem'), may hold values from 0.5 to 1.5
- w_query: bfloat16 [4, 896, 896], P('mem'), may hold values from -1.5 to 1.5
- w_keyval: bfloat16 [4, 896, 256], P('mem'), may hold values from -0.5 to 0.5
- w_out: bfloat16 [4, 896, 896], P('mem'), may hold values from -0.1875 to 0.1875
- server_gain: float32 [8, 896], P('grp'), may hold values from 0.5 to 1.5
- w_gate: bfloat16 [8, 896, 4864], P('grp', None, 'mem'), may hold values from -0.1875 to 0.1875
- w_up: bfloat16 [8, 896, 4864], P('grp', None, 'mem'), may hold values from -0.1875 to 0.1875
- w_down: bfloat16 [8, 4864, 896], P('grp', 'mem'), may hold values from -0.078125 to 0.078125
- out_grad: bfloat16 [8, 4, 128, 896], P('grp', 'mem'), may hold values from -6 to 6
- valid: int32 [8, 4], P('grp', 'mem'), may hold values from 64 to 128
Outputs:
- server_out: bfloat16 [8, 4, 128, 896], P('grp', 'mem')
- grad_query: bfloat16 [4, 896, 896], P('mem')
- grad_keyval: bfloat16 [4, 896, 256], P('mem')
- grad_out: bfloat16 [4, 896, 896], P('mem')
- grad_gate: bfloat16 [8, 896, 4864], P('grp', None, 'mem')
- grad_up: bfloat16 [8, 896, 4864], P('grp', None, 'mem')
- grad_down: bfloat16 [8, 4864, 896], P('grp', 'mem')
The draws below stay inside these ranges and needn't reach their ends.
All inputs are finite; a program needn't handle non-finite values.
Results may differ from the reference program's by a relative error of at most 0.03.
Values may be sent and summed in bfloat16 or wider, within the bound.
A program may use at most 128 MiB of HBM per device.

```python
import jax
import jax.numpy as jnp
from jax import lax

D = 896
FF = 4864
KV_HEADS = 2
HEAD_DIM = 64
TOK = 128
GROUPS = 8
MEMBERS = 4


def query_tables(key):
    first, second = jax.random.split(jax.random.fold_in(key, 11))
    scale = D ** (-0.5)
    keyval = jax.random.normal(first, (MEMBERS, D, 2 * KV_HEADS * HEAD_DIM), jnp.float32) * scale
    query = jax.random.normal(second, (MEMBERS, D, D), jnp.float32) * scale
    return (jnp.clip(query, -1.5, 1.5), jnp.clip(keyval, -0.5, 0.5))


def draw_w_query(key, part):
    return query_tables(key)[0].astype(jnp.bfloat16)


def draw_w_keyval(key, part):
    return query_tables(key)[1].astype(jnp.bfloat16)


def touch_ends(drawn, stream_key, least, high):
    dims = drawn.shape
    index_at = [jax.random.randint(jax.random.fold_in(stream_key, axis), (), 0, dims[axis]) for axis in range(len(dims))]
    drawn = drawn.at[tuple(index_at)].set(least)
    longest = dims.index(max(dims))
    index_at[longest] = (index_at[longest] + 1) % dims[longest]
    return drawn.at[tuple(index_at)].set(high)


def shard_levels(key, extent, pieces, smallest, largest):
    gain, own = 1.0, jax.random.fold_in(key, 6)
    for axis_at, shards_of in pieces:
        steps = jnp.exp(jax.random.uniform(jax.random.fold_in(own, axis_at), (shards_of,), jnp.float32, smallest / len(pieces), largest / len(pieces)))
        gain = gain * jnp.repeat(steps, extent[axis_at] // shards_of).reshape([-1 if axis == axis_at else 1 for axis in range(len(extent))])
    return gain


def scatter_about(own_key, dims, scale, limit, pieces=(), held_as=jnp.bfloat16):
    values = scale * jax.random.normal(own_key, dims, jnp.float32)
    if pieces:
        values = values * shard_levels(own_key, dims, pieces, -0.22, 0.18)
    return jnp.clip(values, -limit, limit).astype(held_as)


def setup_inputs(seed: int = 0) -> dict:
    keys = jax.random.split(jax.random.key(seed), 12)
    return {
        "client_input": scatter_about(keys[0], (GROUPS, MEMBERS, TOK, D), 1.0, 6.0, ((0, 8), (1, 4))),
        "client_gain": jnp.clip(1.0 + 0.1 * jax.random.normal(keys[1], (MEMBERS, D), jnp.float32), 0.5, 1.5),
        "w_query": draw_w_query(jax.random.fold_in(keys[11], 71), 0),
        "w_keyval": draw_w_keyval(jax.random.fold_in(keys[11], 71), 0),
        "w_out": scatter_about(keys[4], (MEMBERS, D, D), D ** -0.5, 0.1875, ((0, 4),)),
        "server_gain": jnp.clip(1.0 + 0.1 * jax.random.normal(keys[5], (GROUPS, D), jnp.float32), 0.5, 1.5),
        "w_gate": scatter_about(keys[6], (GROUPS, D, FF), D ** -0.5, 0.1875, ((0, 8), (2, 4))),
        "w_up": scatter_about(keys[7], (GROUPS, D, FF), D ** -0.5, 0.1875, ((0, 8), (2, 4))),
        "w_down": scatter_about(keys[8], (GROUPS, FF, D), FF ** -0.5, 0.078125, ((0, 8), (1, 4))),
        "out_grad": scatter_about(keys[9], (GROUPS, MEMBERS, TOK, D), 1.0, 6.0, ((0, 8), (1, 4))),
        "valid": touch_ends(jax.random.randint(keys[10], (GROUPS, MEMBERS), TOK // 2, TOK + 1), jax.random.fold_in(keys[10], 1), TOK // 2, TOK).astype(jnp.int32),
    }


EPS = 1e-06

def client_forward(tokens_in, gain_vec, query_w, keyval_w, output_w):
    x_float = tokens_in.astype(jnp.float32)
    inv_rms = lax.rsqrt(lax.optimization_barrier(jnp.mean(x_float * x_float, axis=-1, keepdims=True)) + EPS)
    normed = (x_float * inv_rms * gain_vec).astype(jnp.bfloat16)
    queries = jnp.dot(normed, query_w, preferred_element_type=jnp.float32).astype(jnp.bfloat16)
    key_vals = jnp.dot(normed, keyval_w, preferred_element_type=jnp.float32).astype(jnp.bfloat16)
    length = tokens_in.shape[0]
    half_cols = KV_HEADS * HEAD_DIM
    q_heads = queries.reshape(length, KV_HEADS, -1, HEAD_DIM)
    k_heads = key_vals[:, :half_cols].reshape(length, KV_HEADS, HEAD_DIM)
    v_heads = key_vals[:, half_cols:].reshape(length, KV_HEADS, HEAD_DIM)
    scores = jnp.einsum('tgqd,sgd->gqts', q_heads.astype(jnp.float32), k_heads.astype(jnp.float32)) * HEAD_DIM ** (-0.5)
    causal = jnp.arange(length)[:, None] >= jnp.arange(length)[None, :]
    scores = jnp.where(causal, scores, -1e+30)
    highest = lax.optimization_barrier(jnp.max(scores, axis=-1, keepdims=True))
    expo = jnp.exp(scores - highest)
    probs = (expo / lax.optimization_barrier(jnp.sum(expo, axis=-1, keepdims=True))).astype(jnp.bfloat16)
    attended = jnp.einsum('gqts,sgd->tgqd', probs.astype(jnp.float32), v_heads.astype(jnp.float32))
    attended = attended.astype(jnp.bfloat16).reshape(length, -1)
    mixed = jnp.dot(attended, output_w, preferred_element_type=jnp.float32)
    return (x_float + mixed).astype(jnp.bfloat16)

def client_gradients(tokens_in, gain_vec, query_w, keyval_w, output_w, upstream):

    def inner(query_in, keyval_in, output_in):
        return client_forward(tokens_in, gain_vec, query_in, keyval_in, output_in)
    _, pull = jax.vjp(inner, query_w, keyval_w, output_w)
    return pull(upstream)

def norm_back(h_float, inv_rms, gain_vec, upstream):
    scaled = upstream * gain_vec
    return inv_rms * scaled - h_float * inv_rms ** 3 * lax.optimization_barrier(jnp.mean(scaled * h_float, axis=-1, keepdims=True))

def reference(client_input, client_gain, w_query, w_keyval, w_out, server_gain, w_gate, w_up, w_down, out_grad, valid):
    groups = client_input.shape[0]
    members = client_input.shape[1]
    length = client_input.shape[2]
    width = client_input.shape[3]
    positions = jnp.arange(length).astype(jnp.int32)

    def group_step(totals, group_in):
        x_group, s_gain, gate_w, up_w, down_w, cot_group, valid_group = group_in
        cuts = jax.vmap(client_forward)(x_group, client_gain, w_query, w_keyval, w_out)
        rows_cut = cuts.reshape(-1, width)
        h_float = rows_cut.astype(jnp.float32)
        inv_rms = lax.rsqrt(lax.optimization_barrier(jnp.mean(h_float * h_float, axis=-1, keepdims=True)) + EPS)
        normed = (h_float * inv_rms * s_gain).astype(jnp.bfloat16)
        gate_act = jnp.dot(normed, gate_w, preferred_element_type=jnp.float32)
        up_act = jnp.dot(normed, up_w, preferred_element_type=jnp.float32)
        sigma = jax.nn.sigmoid(gate_act)
        hidden = (gate_act * sigma * up_act).astype(jnp.bfloat16)
        server_rows = (h_float + jnp.dot(hidden, down_w, preferred_element_type=jnp.float32)).astype(jnp.bfloat16)
        live = positions[None, :] < valid_group[:, None]
        cot_rows = jnp.where(live[:, :, None], cot_group, jnp.zeros_like(cot_group)).reshape(-1, width)
        d_hidden = jnp.dot(cot_rows, down_w.T, preferred_element_type=jnp.float32)
        d_gate = (d_hidden * up_act * sigma * (1.0 + gate_act * (1.0 - sigma))).astype(jnp.bfloat16)
        d_up = (d_hidden * gate_act * sigma).astype(jnp.bfloat16)
        grad_down = jnp.dot(hidden.T, cot_rows, preferred_element_type=jnp.float32).astype(jnp.bfloat16)
        grad_gate = jnp.dot(normed.T, d_gate, preferred_element_type=jnp.float32).astype(jnp.bfloat16)
        grad_up = jnp.dot(normed.T, d_up, preferred_element_type=jnp.float32).astype(jnp.bfloat16)
        d_normed = jnp.dot(d_gate, gate_w.T, preferred_element_type=jnp.float32) + jnp.dot(d_up, up_w.T, preferred_element_type=jnp.float32)
        d_cut = cot_rows.astype(jnp.float32) + norm_back(h_float, inv_rms, s_gain, d_normed)
        cut_grad = (lax.optimization_barrier(jnp.sum(d_cut.reshape(members, length, width), axis=0)) / members).astype(jnp.bfloat16)
        grads = jax.vmap(client_gradients, in_axes=(0, 0, 0, 0, 0, None))(x_group, client_gain, w_query, w_keyval, w_out, cut_grad)
        new_totals = tuple((total + lax.optimization_barrier(piece).astype(jnp.float32) for total, piece in zip(totals, grads)))
        return (new_totals, (server_rows.reshape(members, length, width), grad_gate, grad_up, grad_down))
    start = (jnp.zeros(w_query.shape, jnp.float32), jnp.zeros(w_keyval.shape, jnp.float32), jnp.zeros(w_out.shape, jnp.float32))
    totals, stacked = lax.scan(group_step, start, (client_input, server_gain, w_gate, w_up, w_down, out_grad, valid))
    server_out, grad_gate, grad_up, grad_down = stacked
    grad_query = (totals[0] / groups).astype(jnp.bfloat16)
    grad_keyval = (totals[1] / groups).astype(jnp.bfloat16)
    grad_out = (totals[2] / groups).astype(jnp.bfloat16)
    return (server_out, grad_query, grad_keyval, grad_out, grad_gate, grad_up, grad_down)
```

```python
import jax
import jax.numpy as jnp
from jax import lax
from jax.experimental import pallas as pl
from jax.experimental.pallas import tpu as pltpu
from jax.sharding import PartitionSpec as P

KV_HEADS = 2
HEAD_DIM = 64


EPS = 1e-06
F32 = jnp.float32
BF16 = jnp.bfloat16
CONTRACT_LAST = (((1,), (1,)), ((), ()))
CONTRACT_FIRST = (((0,), (0,)), ((), ()))
FIRST_WITH_LAST = (((0,), (1,)), ((), ()))
MESH = pl.DeviceIdType.MESH
SCALE = HEAD_DIM ** (-0.5)


def rms(h_float):
    return lax.rsqrt(jnp.mean(h_float * h_float, axis=-1, keepdims=True) + EPS)


def norm_back(h_float, inv_rms, gain_vec, upstream):
    scaled = upstream * gain_vec
    return inv_rms * scaled - h_float * inv_rms**3 * jnp.mean(
        scaled * h_float, axis=-1, keepdims=True
    )


def dot(left, right, dims=(((1,), (0,)), ((), ()))):
    return lax.dot_general(left, right, dims, preferred_element_type=F32)


class Gather:
    def __init__(self, axis, slot, rows, sems, split=False):
        self.axis, self.slot, self.rows, self.sems = axis, slot, rows, sems
        self.taken = set()
        self.n = lax.axis_size(axis)
        self.pairs = self.n // 2
        me = lax.axis_index(axis)
        self.right = {axis: lax.rem(me + 2, self.n)}
        self.partner = {axis: me + 1 - 2 * lax.rem(me, 2)}
        self.split = split and self.pairs > 1
        self.cut_at = rows // 2

    def send(self, src, dst, first, index, device):
        return pltpu.make_async_remote_copy(
            src_ref=src,
            dst_ref=dst,
            send_sem=self.sems[first].at[index],
            recv_sem=self.sems[first + 1].at[index],
            device_id=device,
            device_id_type=MESH,
        )

    def ring_copy(self, step):
        src, dst = self.slot(2 * step, 0, self.rows), self.slot(2 * step + 2, 0, self.rows)
        return self.send(src, dst, 0, step, self.right)

    def rest_copy(self):
        last, low, count = 2 * self.pairs - 1, self.cut_at, self.rows - self.cut_at
        src, dst = self.slot(last - 2, low, count), self.slot(last, low, count)
        return self.send(src, dst, 0, self.pairs - 1, self.right)

    def flip_copy(self, step):
        rows = self.cut_at if self.split and step == self.pairs - 1 else self.rows
        src, dst = self.slot(2 * step, 0, rows), self.slot(2 * step + 1, 0, rows)
        return self.send(src, dst, 2, step, self.partner)

    def advance(self, step):
        if step > 0:
            self.ring_copy(step - 1).wait_recv()
        if step < self.pairs - 1:
            self.ring_copy(step).start()
        self.flip_copy(step).start()
        if self.split and step == self.pairs - 1:
            self.take(step - 1)
            self.rest_copy().start()

    def take(self, step):
        if step in self.taken:
            return
        self.taken.add(step)
        self.flip_copy(step).wait_recv()
        if self.split and step == self.pairs - 1:
            self.rest_copy().wait_recv()

    def finish(self):
        for step in range(self.pairs):
            if step < self.pairs - 1:
                self.ring_copy(step).wait_send()
            self.flip_copy(step).wait_send()
        if self.split:
            self.rest_copy().wait_send()


def gather_sems(n):
    return [pltpu.SemaphoreType.DMA((n // 2,))] * 4


def greet(axes):
    barrier = pltpu.get_barrier_semaphore()
    count = 0
    for axis in axes:
        n = lax.axis_size(axis)
        me = lax.axis_index(axis)
        pl.semaphore_signal(
            barrier, 1, device_id={axis: me + 1 - 2 * lax.rem(me, 2)}, device_id_type=MESH
        )
        for k in range(1, n // 2):
            pl.semaphore_signal(
                barrier, 1, device_id={axis: lax.rem(me + 2 * k, n)}, device_id_type=MESH
            )
        count += n // 2
    pl.semaphore_wait(barrier, count)


def send(src, dst, sems, index, device):
    return pltpu.make_async_remote_copy(
        src_ref=src,
        dst_ref=dst,
        send_sem=sems[0].at[index],
        recv_sem=sems[1].at[index],
        device_id=device,
        device_id_type=MESH,
    )


def step_kernel(
    x_own, og_own, valid, c_gain, s_gain, wq_far, wkv_far, wo_far, gate_far, up_far, down_far,
    server_out_far, g_gate_far, g_up_far, g_down_far, normed_far, att_far, dqkv_far, cg_far,
    wq, wkv, wo, gate_w, up_w, down_w,
    normed_all, q_all, kv_all, p_all, att_all, dqkv_all, cg_all,
    cut_slots, rows_cot, rows_normed, hidden, d_gate, d_up, g_gate, g_up, g_down,
    served, served_in, home_in, home_out, sums, result, give, give_in, passing, pass_in,
    load_sem, store_sem, early_sems, late_sems, cut_sems, cot_sems,
    swap_sems, part_sems, home_sems, pass_sems, half_sems,
):
    members, groups = lax.axis_size("mem"), lax.axis_size("grp")
    pairs, group_pairs = members // 2, groups // 2
    length, width = x_own.shape
    half = length // 2
    me = lax.axis_index("mem")
    odd = lax.rem(me, 2)
    partner = {"mem": me + 1 - 2 * odd}
    q_cols = wq.shape[1]
    per_kv = q_cols // HEAD_DIM // KV_HEADS
    kv_rows = KV_HEADS * HEAD_DIM

    loads = {}
    for i, (name, far, near) in enumerate((
        ("wq", wq_far, wq), ("wkv", wkv_far, wkv), ("wo", wo_far, wo),
        ("down", down_far, down_w), ("gate", gate_far, gate_w), ("up", up_far, up_w),
    )):
        loads[name] = pltpu.make_async_copy(far, near, load_sem.at[i])
        loads[name].start()
    stores = []

    def store(near, far):
        stores.append(pltpu.make_async_copy(near, far, store_sem.at[len(stores)]))
        stores[-1].start()

    keep_at = pl.multiple_of(odd * half, half)
    give_at = pl.multiple_of((1 - odd) * half, half)

    def half_slot(index, low, count):
        return cg_all.at[index, pl.ds(pl.multiple_of(keep_at + low, 8), count)]

    def whole(ref):
        return lambda index, low, count: ref.at[index, pl.ds(low, count)]

    cut = Gather("mem", whole(cut_slots), length, cut_sems)
    cot = Gather("mem", whole(rows_cot), length, cot_sems)
    early = Gather("grp", whole(normed_all), length, early_sems, True)
    late = Gather("grp", half_slot, half, late_sems, True)

    live = lax.broadcasted_iota(jnp.int32, (length, width), 0) < valid[0, 0]
    own_cot = jnp.where(live, og_own[...].astype(F32), 0.0)
    rows_cot[0] = own_cot.astype(BF16)
    sums[...] = own_cot
    x_float = x_own[...].astype(F32)
    normed_all[0] = (x_float * rms(x_float) * c_gain[...]).astype(BF16)
    greet(("grp", "mem"))
    cot.advance(0)
    early.advance(0)

    key_at = lax.broadcasted_iota(jnp.int32, (length, length), 0)
    query_at = lax.broadcasted_iota(jnp.int32, (length, length), 1)
    bias = jnp.where(key_at <= query_at, 0.0, -1e30).astype(F32)
    bias = jnp.concatenate([bias] * per_kv, axis=1)

    def side_by_side(rows, kv):
        first = kv * per_kv * HEAD_DIM
        return jnp.concatenate(
            [rows[first + i * HEAD_DIM : first + (i + 1) * HEAD_DIM] for i in range(per_kv)], axis=1
        )

    def stacked(columns):
        return jnp.concatenate(
            [columns[:, i * length : (i + 1) * length] for i in range(per_kv)], axis=0
        )

    def forward(first, count):
        normed = normed_all[pl.ds(first, count)].reshape(count * length, width)
        queries = (dot(normed, wq[...]) * SCALE).astype(BF16).T
        key_vals = dot(normed, wkv[...]).astype(BF16).T
        for i in range(count):
            slot, span = first + i, slice(i * length, (i + 1) * length)
            kv_all[slot] = key_vals[:, span]
            for kv in range(KV_HEADS):
                keys = key_vals[kv * HEAD_DIM : (kv + 1) * HEAD_DIM, span]
                vals = key_vals[kv_rows + kv * HEAD_DIM : kv_rows + (kv + 1) * HEAD_DIM, span]
                q_cat = side_by_side(queries[:, span], kv)
                q_all[slot, kv] = q_cat
                scores = dot(keys, q_cat, CONTRACT_FIRST) + bias
                expo = jnp.exp(scores - jnp.max(scores, axis=0, keepdims=True))
                probs = (expo * (1.0 / jnp.sum(expo, axis=0, keepdims=True))).astype(BF16)
                p_all[slot, kv] = probs
                att_all[
                    pl.ds(kv * per_kv * HEAD_DIM, per_kv * HEAD_DIM), pl.ds(slot * length, length)
                ] = stacked(dot(vals, probs).astype(BF16))

    def backward(first, count):
        upstream = cg_all[pl.ds(first, count)].reshape(count * length, width)
        d_att = dot(wo[...], upstream, CONTRACT_LAST).astype(BF16)
        for i in range(count):
            slot, span = first + i, slice(i * length, (i + 1) * length)
            columns = pl.ds(slot * length, length)
            for kv in range(KV_HEADS):
                keys = kv_all[slot, pl.ds(kv * HEAD_DIM, HEAD_DIM)]
                vals = kv_all[slot, pl.ds(kv_rows + kv * HEAD_DIM, HEAD_DIM)]
                d_cat = side_by_side(d_att[:, span], kv)
                probs = p_all[slot, kv]
                weighed = dot(vals, d_cat, CONTRACT_FIRST)
                p_float = probs.astype(F32)
                weighed = weighed * p_float
                d_scores = weighed - p_float * jnp.sum(weighed, axis=0, keepdims=True)
                d_scores = d_scores.astype(BF16)
                d_q = (dot(keys, d_scores) * SCALE).astype(BF16)
                dqkv_all[pl.ds(kv * per_kv * HEAD_DIM, per_kv * HEAD_DIM), columns] = stacked(d_q)
                dqkv_all[pl.ds(q_cols + kv * HEAD_DIM, HEAD_DIM), columns] = dot(
                    q_all[slot, kv], d_scores, CONTRACT_LAST
                ).astype(BF16)
                dqkv_all[pl.ds(q_cols + kv_rows + kv * HEAD_DIM, HEAD_DIM), columns] = dot(
                    d_cat, probs, CONTRACT_LAST
                ).astype(BF16)

    loads["wq"].wait()
    loads["wkv"].wait()
    forward(0, 1)
    loads["wo"].wait()
    mixed = dot(att_all[:, pl.ds(0, length)], wo[...], CONTRACT_FIRST)
    cut_slots[0] = (x_own[...].astype(F32) + mixed).astype(BF16)
    cut.advance(0)

    early_steps = list(range(1, group_pairs))
    ready = [1, 1]

    def keep_going():
        if early_steps:
            step = early_steps.pop(0)
            early.advance(step)
            ready[1] = 2 * step

    def recompute(limit):
        while ready[0] < min(limit, groups):
            first = ready[0]
            count = 1 if first % 2 else 2
            early.take((first + count - 1) // 2)
            forward(first, count)
            ready[0] += count

    for p in range(pairs):
        if p > 0:
            cut.advance(p)
            cot.advance(p)
        cut.take(p)
        cot.take(p)
        span = pl.ds(2 * p, 2)
        h_float = cut_slots[span].reshape(2 * length, width).astype(F32)
        inv_rms = rms(h_float)
        normed = (h_float * inv_rms * s_gain[...]).astype(BF16)
        rows_normed[span] = normed.reshape(2, length, width)
        if p == 0:
            for name in ("down", "gate", "up"):
                loads[name].wait()
        d_hidden = dot(rows_cot[span].reshape(2 * length, width), down_w[...], CONTRACT_LAST)
        gate_act = dot(normed, gate_w[...], CONTRACT_LAST)
        up_act = dot(normed, up_w[...], CONTRACT_LAST)
        if p > 0:
            keep_going()
        sigma = jax.nn.sigmoid(gate_act)
        acted = gate_act * sigma
        hidden_now = (acted * up_act).astype(BF16)
        dg = (d_hidden * up_act * sigma * (1.0 + gate_act * (1.0 - sigma))).astype(BF16)
        du = (d_hidden * acted).astype(BF16)
        rows = pl.ds(2 * p * length, 2 * length)
        hidden[rows] = hidden_now
        d_gate[rows] = dg
        d_up[rows] = du
        d_normed = dot(dg, gate_w[...]) + dot(du, up_w[...])
        pushed = norm_back(h_float, inv_rms, s_gain[...], d_normed)
        sums[...] += pushed[:length] + pushed[length:]
        served[span] = dot(hidden_now, down_w[...]).astype(BF16).reshape(2, length, width)
        if p == 0:
            keep_going()
            recompute(2)

    give[...] = sums[pl.ds(give_at, half)].astype(BF16)
    handed = send(give, give_in, part_sems, 0, partner)
    handed.start()
    swaps = []
    for p in range(pairs):
        swaps.append(send(served.at[2 * p + 1], served_in.at[p], swap_sems, p, partner))
        swaps[-1].start()
    handed.wait_recv()
    total = sums[pl.ds(keep_at, half)] + give_in[...].astype(F32)
    passing[...] = total.astype(BF16)
    passes = []
    for k in range(1, pairs):
        passes.append(
            send(passing, pass_in.at[k - 1], pass_sems, k - 1, {"mem": lax.rem(me + 2 * k, members)})
        )
        passes[-1].start()
    keep_going()
    recompute(4)
    homes = []
    for p in range(pairs):
        swaps[p].wait_recv()
        mine = served[2 * p].astype(F32) + served_in[p].astype(F32)
        if p == 0:
            result[...] = cut_slots[0].astype(F32) + mine
        else:
            home_out[p - 1] = mine.astype(BF16)
            homes.append(
                send(
                    home_out.at[p - 1], home_in.at[p - 1], home_sems, p - 1,
                    {"mem": lax.rem(me + members - 2 * p, members)},
                )
            )
            homes[-1].start()
    for k in range(1, pairs):
        passes[k - 1].wait_recv()
        total = total + pass_in[k - 1].astype(F32)
    cg_all[0, pl.ds(keep_at, half)] = (total / members).astype(BF16)

    exchanged = {}

    def exchange(slot):
        ref = half_slot(slot, 0, half)
        exchanged[slot] = send(ref, ref, half_sems, slot, partner)
        exchanged[slot].start()

    late.advance(0)
    exchange(0)
    keep_going()

    def weight_grad(left, right, near, far):
        rows = right.shape[0] * length
        near[...] = dot(left[...], right[...].reshape(rows, width), CONTRACT_FIRST).astype(BF16)
        store(near, far)

    weight_grads = [
        (hidden, rows_cot, g_down, g_down_far),
        (d_gate, rows_normed, g_gate, g_gate_far),
        (d_up, rows_normed, g_up, g_up_far),
    ]

    def more():
        if weight_grads:
            weight_grad(*weight_grads.pop(0))

    recompute(6)
    more()
    while early_steps:
        keep_going()
    for step in range(1, group_pairs):
        late.advance(step)
        exchange(2 * step)
        late.take(step - 1)
        exchange(2 * step - 1)
        recompute(groups if step > 1 else 6)
        more()
        if step == 1:
            for p in range(1, pairs):
                homes[p - 1].wait_recv()
                result[...] += home_in[p - 1].astype(F32)
            served[0] = result[...].astype(BF16)
            store(served.at[0], server_out_far)
        if step > 1:
            for slot in (2 * step - 4, 2 * step - 3):
                exchanged[slot].wait_recv()
            backward(2 * step - 4, 2)
    while early_steps:
        keep_going()
    recompute(groups)
    while weight_grads:
        more()
    store(normed_all, normed_far)
    store(att_all, att_far)
    late.take(group_pairs - 1)
    exchange(groups - 1)
    for first in range(max(groups - 4, 0), groups, 2):
        for slot in (first, first + 1):
            exchanged[slot].wait_recv()
        backward(first, 2)
    store(cg_all, cg_far)
    store(dqkv_all, dqkv_far)
    early.finish()
    late.finish()
    cut.finish()
    cot.finish()
    for copy in [handed] + swaps + passes + homes + list(exchanged.values()):
        copy.wait_send()
    for copy in stores:
        copy.wait()


def step_call(x, og, valid, c_gain, s_gain, wq, wkv, wo, gate_t, up_t, down):
    members, groups = lax.axis_size("mem"), lax.axis_size("grp")
    pairs = members // 2
    length, width = x.shape
    units = down.shape[0]
    q_cols, kv_cols = wq.shape[1], wkv.shape[1]
    per_kv = q_cols // HEAD_DIM // KV_HEADS
    half = length // 2
    rows = members * length
    tokens = groups * length
    shape = jax.ShapeDtypeStruct
    near = pl.BlockSpec(memory_space=pltpu.VMEM)
    far = pl.BlockSpec(memory_space=pl.ANY)
    others = max(pairs - 1, 1)
    two = lambda count: [pltpu.SemaphoreType.DMA((count,))] * 2
    vmem = lambda *dims: pltpu.VMEM(dims, BF16)
    return pl.pallas_call(
        step_kernel,
        out_shape=[
            shape((length, width), BF16),
            shape((units, width), BF16),
            shape((units, width), BF16),
            shape((units, width), BF16),
            shape((groups, length, width), BF16),
            shape((q_cols, tokens), BF16),
            shape((q_cols + kv_cols, tokens), BF16),
            shape((groups, length, width), BF16),
        ],
        in_specs=[near] * 2 + [pl.BlockSpec(memory_space=pltpu.SMEM)] + [near] * 2 + [far] * 6,
        out_specs=[far] * 8,
        scratch_shapes=[
            vmem(*wq.shape), vmem(*wkv.shape), vmem(*wo.shape),
            vmem(units, width), vmem(units, width), vmem(units, width),
            vmem(groups, length, width),
            vmem(groups, KV_HEADS, HEAD_DIM, per_kv * length),
            vmem(groups, kv_cols, length),
            vmem(groups, KV_HEADS, length, per_kv * length),
            vmem(q_cols, tokens),
            vmem(q_cols + kv_cols, tokens),
            vmem(groups, length, width),
            vmem(members, length, width), vmem(members, length, width), vmem(members, length, width),
            vmem(rows, units), vmem(rows, units), vmem(rows, units),
            vmem(units, width), vmem(units, width), vmem(units, width),
            vmem(members, length, width),
            vmem(pairs, length, width),
            vmem(others, length, width),
            vmem(others, length, width),
            pltpu.VMEM((length, width), F32),
            pltpu.VMEM((length, width), F32),
            vmem(half, width), vmem(half, width), vmem(half, width),
            vmem(others, half, width),
            pltpu.SemaphoreType.DMA((6,)),
            pltpu.SemaphoreType.DMA((8,)),
            gather_sems(groups), gather_sems(groups), gather_sems(members), gather_sems(members),
            two(pairs), two(1), two(others), two(others), two(groups),
        ],
        compiler_params=pltpu.CompilerParams(
            collective_id=0, has_side_effects=True, vmem_limit_bytes=67043328
        ),
        name="step",
    )(x, og, valid, c_gain, s_gain, wq, wkv, wo, gate_t, up_t, down)


def grads_kernel(
    groups, server_far, gate_far, up_far, down_far, normed_far, att_far, dqkv_far, cg_far,
    server_out, g_query_out, g_keyval_out, g_out_out, g_gate_out, g_up_out, g_down_out,
    server, gate, up, down, normed, att, dqkv, cg, g_query, g_keyval, g_out, load_sem, store_sem,
):
    tokens = att.shape[1]
    width = normed.shape[2]
    columns = g_query.shape[1]
    loads = {}
    for i, (name, source, near) in enumerate((
        ("att", att_far, att), ("cg", cg_far, cg), ("normed", normed_far, normed),
        ("dqkv", dqkv_far, dqkv), ("down", down_far, down), ("gate", gate_far, gate),
        ("up", up_far, up), ("server", server_far, server),
    )):
        loads[name] = pltpu.make_async_copy(source, near, load_sem.at[i])
        loads[name].start()
    stores = []

    def store(near, out):
        stores.append(pltpu.make_async_copy(near, out, store_sem.at[len(stores)]))
        stores[-1].start()

    scale = 1.0 / groups
    loads["att"].wait()
    loads["cg"].wait()
    g_out[...] = (dot(att[...], cg[...].reshape(tokens, width)) * scale).astype(BF16)
    store(g_out, g_out_out)
    loads["normed"].wait()
    loads["dqkv"].wait()
    for name, near, out in (("down", down, g_down_out), ("gate", gate, g_gate_out)):
        loads[name].wait()
        store(near, out)
    grads = dot(normed[...].reshape(tokens, width), dqkv[...], FIRST_WITH_LAST) * scale
    g_query[...] = grads[:, :columns].astype(BF16)
    store(g_query, g_query_out)
    g_keyval[...] = grads[:, columns:].astype(BF16)
    store(g_keyval, g_keyval_out)
    for name, near, out in (("up", up, g_up_out), ("server", server, server_out)):
        loads[name].wait()
        store(near, out)
    for copy in stores:
        copy.wait()


def grads_call(columns, *arrays):
    server, gate, up, down, normed, att, dqkv, cg = arrays
    groups, _, width = normed.shape
    wide = dqkv.shape[0]
    far = pl.BlockSpec(memory_space=pl.ANY)
    outs = [
        server.shape, (width, columns), (width, wide - columns), (att.shape[0], width),
        gate.shape, up.shape, down.shape,
    ]
    return pl.pallas_call(
        lambda *refs: grads_kernel(groups, *refs),
        out_shape=[jax.ShapeDtypeStruct(o, BF16) for o in outs],
        in_specs=[far] * len(arrays),
        out_specs=[far] * len(outs),
        scratch_shapes=[pltpu.VMEM(a.shape, BF16) for a in arrays]
        + [pltpu.VMEM(o, BF16) for o in outs[1:4]]
        + [pltpu.SemaphoreType.DMA((len(arrays),)), pltpu.SemaphoreType.DMA((len(outs),))],
        compiler_params=pltpu.CompilerParams(vmem_limit_bytes=67043328),
        name="grads",
    )(*arrays)


def on_device(
    client_input,
    client_gain,
    w_query,
    w_keyval,
    w_out,
    server_gain,
    w_gate,
    w_up,
    w_down,
    out_grad,
    valid,
):
    server, gate, up, down, normed, att, dqkv, cg = step_call(
        client_input[0, 0], out_grad[0, 0], valid, client_gain, server_gain,
        w_query[0], w_keyval[0], w_out[0], w_gate[0].T, w_up[0].T, w_down[0],
    )
    (server_out, grad_query, grad_keyval, grad_out, grad_gate, grad_up, grad_down) = grads_call(
        w_query.shape[2], server, gate, up, down, normed, att, dqkv, cg
    )
    return (
        server_out[None, None],
        grad_query[None],
        grad_keyval[None],
        grad_out[None],
        grad_gate.T[None],
        grad_up.T[None],
        grad_down[None],
    )


def solution(mesh):
    in_specs = (
        P("grp", "mem", None, None),
        P("mem", None),
        P("mem", None, None),
        P("mem", None, None),
        P("mem", None, None),
        P("grp", None),
        P("grp", None, "mem"),
        P("grp", None, "mem"),
        P("grp", "mem", None),
        P("grp", "mem", None, None),
        P("grp", "mem"),
    )
    out_specs = (
        P("grp", "mem", None, None),
        P("mem", None, None),
        P("mem", None, None),
        P("mem", None, None),
        P("grp", None, "mem"),
        P("grp", None, "mem"),
        P("grp", "mem", None),
    )
    return jax.shard_map(
        on_device, mesh=mesh, in_specs=in_specs, out_specs=out_specs, check_vma=False
    )
```

```python
import functools
import math

import jax
import jax.numpy as jnp
from jax import lax
from jax.experimental import pallas as pl
from jax.experimental.pallas import tpu as pltpu
from jax.sharding import PartitionSpec as P

KV_HEADS = 2
HEAD_DIM = 64


EPS = 1e-06
VMEM_MOST = 67043328
F32 = jnp.float32
BF16 = jnp.bfloat16
CONTRACT_LAST = (((1,), (1,)), ((), ()))
CONTRACT_FIRST = (((0,), (0,)), ((), ()))
FIRST_WITH_LAST = (((0,), (1,)), ((), ()))
MESH = pl.DeviceIdType.MESH
SCALE = HEAD_DIM ** (-0.5)


def rms(h_float):
    return lax.rsqrt(jnp.mean(h_float * h_float, axis=-1, keepdims=True) + EPS)


def norm_back(h_float, inv_rms, gain_vec, upstream):
    scaled = upstream * gain_vec
    return inv_rms * scaled - h_float * inv_rms**3 * jnp.mean(
        scaled * h_float, axis=-1, keepdims=True
    )


def dot(left, right, dims=(((1,), (0,)), ((), ()))):
    return lax.dot_general(left, right, dims, preferred_element_type=F32)


class Gather:
    def __init__(self, axis, slot, rows, sems, split=False):
        self.axis, self.slot, self.rows, self.sems = axis, slot, rows, sems
        self.taken = set()
        self.n = lax.axis_size(axis)
        self.pairs = self.n // 2
        me = lax.axis_index(axis)
        self.right = {axis: lax.rem(me + 2, self.n)}
        self.partner = {axis: me + 1 - 2 * lax.rem(me, 2)}
        self.split = split and self.pairs > 1
        self.cut_at = rows // 2

    def send(self, src, dst, first, index, device):
        return pltpu.make_async_remote_copy(
            src_ref=src,
            dst_ref=dst,
            send_sem=self.sems[first].at[index],
            recv_sem=self.sems[first + 1].at[index],
            device_id=device,
            device_id_type=MESH,
        )

    def ring_copy(self, step):
        src, dst = self.slot(2 * step, 0, self.rows), self.slot(2 * step + 2, 0, self.rows)
        return self.send(src, dst, 0, step, self.right)

    def rest_copy(self):
        last, low, count = 2 * self.pairs - 1, self.cut_at, self.rows - self.cut_at
        src, dst = self.slot(last - 2, low, count), self.slot(last, low, count)
        return self.send(src, dst, 0, self.pairs - 1, self.right)

    def flip_copy(self, step):
        rows = self.cut_at if self.split and step == self.pairs - 1 else self.rows
        src, dst = self.slot(2 * step, 0, rows), self.slot(2 * step + 1, 0, rows)
        return self.send(src, dst, 2, step, self.partner)

    def advance(self, step, ring=True):
        if step > 0:
            self.ring_copy(step - 1).wait_recv()
        if ring:
            self.pass_on(step)
        self.flip_copy(step).start()
        if self.split and step == self.pairs - 1:
            self.take(step - 1)
            self.rest_copy().start()

    def pass_on(self, step):
        if step < self.pairs - 1:
            self.ring_copy(step).start()

    def take(self, step):
        if step in self.taken:
            return
        self.taken.add(step)
        self.flip_copy(step).wait_recv()
        if self.split and step == self.pairs - 1:
            self.rest_copy().wait_recv()

    def finish(self):
        for step in range(self.pairs):
            if step < self.pairs - 1:
                self.ring_copy(step).wait_send()
            self.flip_copy(step).wait_send()
        if self.split:
            self.rest_copy().wait_send()


def gather_sems(n):
    return [pltpu.SemaphoreType.DMA((n // 2,))] * 4


def greet(axes):
    barrier = pltpu.get_barrier_semaphore()
    count = 0
    for axis in axes:
        n = lax.axis_size(axis)
        me = lax.axis_index(axis)
        pl.semaphore_signal(
            barrier, 1, device_id={axis: me + 1 - 2 * lax.rem(me, 2)}, device_id_type=MESH
        )
        for k in range(1, n // 2):
            pl.semaphore_signal(
                barrier, 1, device_id={axis: lax.rem(me + 2 * k, n)}, device_id_type=MESH
            )
        count += n // 2
    return lambda: pl.semaphore_wait(barrier, count)


def send(src, dst, sems, index, device):
    return pltpu.make_async_remote_copy(
        src_ref=src,
        dst_ref=dst,
        send_sem=sems[0].at[index],
        recv_sem=sems[1].at[index],
        device_id=device,
        device_id_type=MESH,
    )


def step_kernel(
    share, x_far, og_far, valid, c_gain, s_gain, wq_far, wkv_far, wo_far, gate_far, up_far, down_far,
    server_out, g_gate, g_up, g_down, normed_all, att_all, dqkv_all, cg_all, g_qkv_part, g_out_part,
    x_own, og_own, wq, wkv, wo, gate_w, up_w, down_w,
    q_all, kv_all, p_all,
    cut_slots, rows_cot, rows_normed, hidden, d_gate, d_up,
    served, served_in, home_in, home_out, sums, result, give, give_in, passing, pass_in,
    load_sem, early_sems, late_sems, cut_sems, cot_sems,
    swap_sems, part_sems, home_sems, pass_sems, half_sems,
):
    members, groups = lax.axis_size("mem"), lax.axis_size("grp")
    pairs, group_pairs = members // 2, groups // 2
    length, width = x_own.shape
    half = length // 2
    me = lax.axis_index("mem")
    odd = lax.rem(me, 2)
    partner = {"mem": me + 1 - 2 * odd}
    q_cols = wq.shape[1]
    per_kv = q_cols // HEAD_DIM // KV_HEADS
    kv_rows = KV_HEADS * HEAD_DIM

    loads = {}
    for i, (name, far, near) in enumerate((
        ("x", x_far, x_own), ("og", og_far, og_own), ("wq", wq_far, wq), ("wkv", wkv_far, wkv), ("wo", wo_far, wo),
        ("down", down_far, down_w), ("gate", gate_far, gate_w), ("up", up_far, up_w),
    )):
        loads[name] = pltpu.make_async_copy(far, near, load_sem.at[i])
        loads[name].start()
    met = greet(("grp", "mem"))

    keep_at = pl.multiple_of(odd * half, half)
    give_at = pl.multiple_of((1 - odd) * half, half)

    def half_slot(index, low, count):
        return cg_all.at[index, pl.ds(pl.multiple_of(keep_at + low, 8), count)]

    def whole(ref, base=0):
        return lambda index, low, count: ref.at[index, pl.ds(base + low, count)]

    cut = Gather("mem", whole(cut_slots), length, cut_sems)
    cot_top = Gather("mem", whole(rows_cot), half, cot_sems[0])
    cot_low = Gather("mem", whole(rows_cot, half), half, cot_sems[1])
    early = Gather("grp", whole(normed_all), length, early_sems, True)
    late = Gather("grp", half_slot, half, late_sems, True)

    for name in ("x", "og"):
        loads[name].wait()
    live = lax.broadcasted_iota(jnp.int32, (length, width), 0) < valid[0, 0]
    own_cot = jnp.where(live, og_own[...].astype(F32), 0.0)
    rows_cot[0] = own_cot.astype(BF16)
    sums[...] = own_cot
    x_float = x_own[...].astype(F32)
    normed_all[0] = (x_float * rms(x_float) * c_gain[...]).astype(BF16)
    with jax.named_scope("greet"):
        met()
    cot_top.advance(0)
    cot_low.advance(0, ring=False)
    early.advance(0)

    key_at = lax.broadcasted_iota(jnp.int32, (length, length), 0)
    query_at = lax.broadcasted_iota(jnp.int32, (length, length), 1)
    bias = jnp.where(key_at <= query_at, 0.0, -1e30).astype(F32)
    bias = jnp.concatenate([bias] * per_kv, axis=1)

    def side_by_side(rows, kv):
        first = kv * per_kv * HEAD_DIM
        return jnp.concatenate(
            [rows[first + i * HEAD_DIM : first + (i + 1) * HEAD_DIM] for i in range(per_kv)], axis=1
        )

    def stacked(columns):
        return jnp.concatenate(
            [columns[:, i * length : (i + 1) * length] for i in range(per_kv)], axis=0
        )

    def forward(first, count):
        normed = normed_all[pl.ds(first, count)].reshape(count * length, width)
        queries = (dot(normed, wq[...]) * SCALE).astype(BF16).T
        key_vals = dot(normed, wkv[...]).astype(BF16).T
        for i in range(count):
            slot, span = first + i, slice(i * length, (i + 1) * length)
            kv_all[slot] = key_vals[:, span]
            for kv in range(KV_HEADS):
                keys = key_vals[kv * HEAD_DIM : (kv + 1) * HEAD_DIM, span]
                vals = key_vals[kv_rows + kv * HEAD_DIM : kv_rows + (kv + 1) * HEAD_DIM, span]
                q_cat = side_by_side(queries[:, span], kv)
                q_all[slot, kv] = q_cat
                scores = dot(keys, q_cat, CONTRACT_FIRST) + bias
                expo = jnp.exp(scores - jnp.max(scores, axis=0, keepdims=True))
                probs = (expo * (1.0 / jnp.sum(expo, axis=0, keepdims=True))).astype(BF16)
                p_all[slot, kv] = probs
                att_all[
                    pl.ds(kv * per_kv * HEAD_DIM, per_kv * HEAD_DIM), pl.ds(slot * length, length)
                ] = stacked(dot(vals, probs).astype(BF16))

    def backward(first, count):
        upstream = cg_all[pl.ds(first, count)].reshape(count * length, width)
        d_att = dot(wo[...], upstream, CONTRACT_LAST).astype(BF16)
        for i in range(count):
            slot, span = first + i, slice(i * length, (i + 1) * length)
            columns = pl.ds(slot * length, length)
            for kv in range(KV_HEADS):
                keys = kv_all[slot, pl.ds(kv * HEAD_DIM, HEAD_DIM)]
                vals = kv_all[slot, pl.ds(kv_rows + kv * HEAD_DIM, HEAD_DIM)]
                d_cat = side_by_side(d_att[:, span], kv)
                probs = p_all[slot, kv]
                weighed = dot(vals, d_cat, CONTRACT_FIRST)
                p_float = probs.astype(F32)
                weighed = weighed * p_float
                d_scores = weighed - p_float * jnp.sum(weighed, axis=0, keepdims=True)
                d_scores = d_scores.astype(BF16)
                d_q = (dot(keys, d_scores) * SCALE).astype(BF16)
                dqkv_all[pl.ds(kv * per_kv * HEAD_DIM, per_kv * HEAD_DIM), columns] = stacked(d_q)
                both = dot(
                    jnp.concatenate([q_all[slot, kv], d_cat], axis=0),
                    jnp.concatenate([d_scores, probs], axis=0),
                    CONTRACT_LAST,
                ).astype(BF16)
                dqkv_all[pl.ds(q_cols + kv * HEAD_DIM, HEAD_DIM), columns] = both[:HEAD_DIM, :length]
                dqkv_all[pl.ds(q_cols + kv_rows + kv * HEAD_DIM, HEAD_DIM), columns] = both[
                    HEAD_DIM:, length:
                ]

    with jax.named_scope("wait_wq"):
        loads["wq"].wait()
        loads["wkv"].wait()
    with jax.named_scope("forward_own"):
        forward(0, 1)
    loads["wo"].wait()
    mixed = dot(att_all[:, pl.ds(0, length)], wo[...], CONTRACT_FIRST)
    cut_slots[0] = (x_own[...].astype(F32) + mixed).astype(BF16)
    cut.advance(0)
    cot_low.pass_on(0)

    early_steps = list(range(1, group_pairs))
    done = {"forward": 1, "backward": 0, "partial": 0}

    def keep_going():
        if early_steps:
            step = early_steps.pop(0)
            with jax.named_scope(f"early_step{step}"):
                early.advance(step)

    def recompute(limit):
        while done["forward"] < min(limit, groups):
            first = done["forward"]
            count = 1 if first % 2 else 2
            step = (first + count - 1) // 2
            while early_steps and early_steps[0] <= step:
                keep_going()
            with jax.named_scope(f"early_take{first}"):
                early.take(step)
            with jax.named_scope(f"forward{first}"):
                forward(first, count)
            done["forward"] += count

    def weight_grad(left, right, near):
        rows = right.shape[0] * length
        near[...] = dot(left[...], right[...].reshape(rows, width), CONTRACT_FIRST).astype(BF16)

    weight_grads = [
        (hidden, rows_cot, g_down), (d_gate, rows_normed, g_gate), (d_up, rows_normed, g_up)
    ]

    def more():
        if weight_grads:
            with jax.named_scope(f"weight_grad{len(weight_grads)}"):
                weight_grad(*weight_grads.pop(0))

    def cot_hidden(p):
        with jax.named_scope(f"wait_cot{p}"):
            for part in (cot_top, cot_low):
                if p > 1 or (p == 1 and part is cot_low):
                    part.advance(p)
            for part in (cot_top, cot_low):
                part.take(p)
        left = rows_cot[pl.ds(2 * p, 2)].reshape(2 * length, width)
        return dot(left, down_w[...], CONTRACT_LAST)

    for p in range(pairs):
        span = pl.ds(2 * p, 2)
        if p == 0:
            loads["down"].wait()
            d_hidden = cot_hidden(0)
        with jax.named_scope(f"wait_cut{p}"):
            if p > 0:
                cut.advance(p)
            cut.take(p)
        h_float = cut_slots[span].reshape(2 * length, width).astype(F32)
        inv_rms = rms(h_float)
        normed = (h_float * inv_rms * s_gain[...]).astype(BF16)
        rows_normed[span] = normed.reshape(2, length, width)
        if p == 0:
            for name in ("gate", "up"):
                loads[name].wait()
        gate_act = dot(normed, gate_w[...], CONTRACT_LAST)
        up_act = dot(normed, up_w[...], CONTRACT_LAST)
        if p > 0:
            d_hidden = cot_hidden(p)
        keep_going()
        sigma = jax.nn.sigmoid(gate_act)
        acted = gate_act * sigma
        hidden_now = (acted * up_act).astype(BF16)
        dg = (d_hidden * up_act * sigma * (1.0 + gate_act * (1.0 - sigma))).astype(BF16)
        du = (d_hidden * acted).astype(BF16)
        rows = pl.ds(2 * p * length, 2 * length)
        hidden[rows] = hidden_now
        d_gate[rows] = dg
        d_up[rows] = du
        d_normed = dot(dg, gate_w[...]) + dot(du, up_w[...])
        pushed = norm_back(h_float, inv_rms, s_gain[...], d_normed)
        sums[...] += pushed[:length] + pushed[length:]
        served[span] = dot(hidden_now, down_w[...]).astype(BF16).reshape(2, length, width)
        if p == 0 and pairs > 1:
            with jax.named_scope("cot_step1"):
                cot_top.advance(1)
        if p == 0:
            recompute(2)

    give[...] = sums[pl.ds(give_at, half)].astype(BF16)
    handed = send(give, give_in, part_sems, 0, partner)
    handed.start()
    swaps = []
    for p in range(pairs):
        swaps.append(send(served.at[2 * p + 1], served_in.at[p], swap_sems, p, partner))
        swaps[-1].start()
    with jax.named_scope("wait_handed"):
        handed.wait_recv()
    total = sums[pl.ds(keep_at, half)] + give_in[...].astype(F32)
    passing[...] = total.astype(BF16)
    passes = []
    for k in range(1, pairs):
        passes.append(
            send(passing, pass_in.at[k - 1], pass_sems, k - 1, {"mem": lax.rem(me + 2 * k, members)})
        )
        passes[-1].start()
    recompute(4)
    keep_going()
    homes = []
    for p in range(pairs):
        with jax.named_scope(f"wait_swap{p}"):
            swaps[p].wait_recv()
        mine = served[2 * p].astype(F32) + served_in[p].astype(F32)
        if p == 0:
            result[...] = cut_slots[0].astype(F32) + mine
        else:
            home_out[p - 1] = mine.astype(BF16)
            homes.append(
                send(
                    home_out.at[p - 1], home_in.at[p - 1], home_sems, p - 1,
                    {"mem": lax.rem(me + members - 2 * p, members)},
                )
            )
            homes[-1].start()
    more()
    for k in range(1, pairs):
        with jax.named_scope(f"wait_pass{k}"):
            passes[k - 1].wait_recv()
        total = total + pass_in[k - 1].astype(F32)
    cg_all[0, pl.ds(keep_at, half)] = (total / members).astype(BF16)

    exchanged = {}

    def exchange(slot):
        ref = half_slot(slot, 0, half)
        exchanged[slot] = send(ref, ref, half_sems, slot, partner)
        exchanged[slot].start()

    def partial_grads(count):
        some = pl.ds(0, count * length)
        normed = normed_all[pl.ds(0, count)].reshape(count * length, width)
        g_qkv_part[...] = dot(normed, dqkv_all[:, some], FIRST_WITH_LAST).astype(BF16)
        upstream = cg_all[pl.ds(0, count)].reshape(count * length, width)
        g_out_part[...] = dot(att_all[:, some], upstream).astype(BF16)

    def pull(limit):
        first = done["backward"]
        while first < limit:
            count = min(4, limit - first)
            recompute(first + count)
            for slot in range(first, first + count):
                with jax.named_scope(f"wait_exchange{slot}"):
                    exchanged[slot].wait_recv()
            with jax.named_scope(f"backward{first}"):
                backward(first, count)
            first += count
        done["backward"] = first

    late.advance(0)
    exchange(0)
    recompute(6)
    more()
    for step in range(1, group_pairs):
        with jax.named_scope(f"late_step{step}"):
            late.advance(step)
        exchange(2 * step)
        with jax.named_scope(f"late_take{step - 1}"):
            late.take(step - 1)
        exchange(2 * step - 1)
        if step == 1:
            recompute(8)
            for p in range(1, pairs):
                with jax.named_scope("wait_home"):
                    homes[p - 1].wait_recv()
                result[...] += home_in[p - 1].astype(F32)
            server_out[...] = result[...].astype(BF16)
        elif step % 2 == 0:
            more()
            pull(2 * step)
        if step == group_pairs - 1 and done["backward"] >= share > 0:
            with jax.named_scope("partial"):
                partial_grads(share)
            done["partial"] = share
    while early_steps:
        keep_going()
    recompute(groups)
    while weight_grads:
        more()
    with jax.named_scope("late_last"):
        late.take(group_pairs - 1)
    exchange(groups - 1)
    pull(groups)
    if not share:
        g_qkv_part[...] = jnp.zeros_like(g_qkv_part)
        g_out_part[...] = jnp.zeros_like(g_out_part)
    elif not done["partial"]:
        partial_grads(share)
    early.finish()
    late.finish()
    cut.finish()
    cot_top.finish()
    cot_low.finish()
    for copy in [handed] + swaps + passes + homes + list(exchanged.values()):
        copy.wait_send()


def step_call(x, og, valid, c_gain, s_gain, wq, wkv, wo, gate_t, up_t, down):
    members, groups = lax.axis_size("mem"), lax.axis_size("grp")
    pairs = members // 2
    length, width = x.shape
    units = down.shape[0]
    q_cols, kv_cols = wq.shape[1], wkv.shape[1]
    per_kv = q_cols // HEAD_DIM // KV_HEADS
    half = length // 2
    rows = members * length
    tokens = groups * length
    kept = [
        (length, width), (units, width), (units, width), (units, width), (groups, length, width),
        (q_cols, tokens), (q_cols + kv_cols, tokens), (groups, length, width),
        (width, q_cols + kv_cols), (q_cols, width),
    ]
    keep = 2 * sum(math.prod(dims) for dims in kept) < 20 * 2**20
    share = groups // 2 if keep else 0
    if not share:
        kept[-2:] = [(16, 128)] * 2
    shape = lambda *dims: pltpu.VMEM(dims, BF16) if keep else jax.ShapeDtypeStruct(dims, BF16)
    near = pl.BlockSpec(memory_space=pltpu.VMEM)
    far = pl.BlockSpec(memory_space=pl.ANY)
    stay = lambda a: pltpu.with_memory_space_constraint(a, pltpu.HBM)
    others = max(pairs - 1, 1)
    two = lambda count: [pltpu.SemaphoreType.DMA((count,))] * 2
    vmem = lambda *dims: pltpu.VMEM(dims, BF16)
    return share, pl.pallas_call(
        functools.partial(step_kernel, share),
        out_shape=[shape(*dims) for dims in kept],
        in_specs=[far] * 2 + [pl.BlockSpec(memory_space=pltpu.SMEM)] + [near] * 2 + [far] * 6,
        out_specs=[near] * 10,
        scratch_shapes=[
            vmem(length, width), vmem(length, width),
            vmem(*wq.shape), vmem(*wkv.shape), vmem(*wo.shape),
            vmem(units, width), vmem(units, width), vmem(units, width),
            vmem(groups, KV_HEADS, HEAD_DIM, per_kv * length),
            vmem(groups, kv_cols, length),
            vmem(groups, KV_HEADS, length, per_kv * length),
            vmem(members, length, width), vmem(members, length, width), vmem(members, length, width),
            vmem(rows, units), vmem(rows, units), vmem(rows, units),
            vmem(members, length, width),
            vmem(pairs, length, width),
            vmem(others, length, width),
            vmem(others, length, width),
            pltpu.VMEM((length, width), F32),
            pltpu.VMEM((length, width), F32),
            vmem(half, width), vmem(half, width), vmem(half, width),
            vmem(others, half, width),
            pltpu.SemaphoreType.DMA((8,)),
            gather_sems(groups), gather_sems(groups), gather_sems(members), [gather_sems(members)] * 2,
            two(pairs), two(1), two(others), two(others), two(groups),
        ],
        compiler_params=pltpu.CompilerParams(
            collective_id=0, has_side_effects=True, vmem_limit_bytes=38 * 2**20 if keep else VMEM_MOST
        ),
        name="step",
    )(stay(x), stay(og), valid, *map(stay, (c_gain, s_gain, wq, wkv, wo, gate_t, up_t, down)))


def grads_kernel(
    share, groups, server, gate, up, down, normed, att, dqkv, cg, qkv_part, out_part,
    server_out, g_query_out, g_keyval_out, g_out_out, g_gate_out, g_up_out, g_down_out,
    g_query, g_keyval, g_out, store_sem,
):
    tokens = att.shape[1]
    width = normed.shape[2]
    columns = g_query.shape[1]
    stores = []

    def store(near, out):
        stores.append(pltpu.make_async_copy(near, out, store_sem.at[len(stores)]))
        stores[-1].start()

    scale = 1.0 / groups
    for near, out in ((down, g_down_out), (gate, g_gate_out), (up, g_up_out), (server, server_out)):
        store(near, out)
    rest = groups - share
    some = pl.ds(tokens - rest * (tokens // groups), rest * (tokens // groups))
    left = normed[pl.ds(groups - rest, rest)].reshape(-1, width)
    grads = dot(left, dqkv[:, some], FIRST_WITH_LAST)
    if share:
        grads = grads + qkv_part[...].astype(F32)
    grads = grads * scale
    g_query[...] = grads[:, :columns].astype(BF16)
    store(g_query, g_query_out)
    g_keyval[...] = grads[:, columns:].astype(BF16)
    store(g_keyval, g_keyval_out)
    right = cg[pl.ds(groups - rest, rest)].reshape(-1, width)
    grads = dot(att[:, some], right)
    if share:
        grads = grads + out_part[...].astype(F32)
    g_out[...] = (grads * scale).astype(BF16)
    store(g_out, g_out_out)
    for copy in stores:
        copy.wait()


def grads_call(share, columns, *arrays):
    server, gate, up, down, normed, att, dqkv, cg, qkv_part, out_part = arrays
    groups, _, width = normed.shape
    wide = dqkv.shape[0]
    far = pl.BlockSpec(memory_space=pl.ANY)
    near = pl.BlockSpec(memory_space=pltpu.VMEM)
    outs = [
        server.shape, (width, columns), (width, wide - columns), (att.shape[0], width),
        gate.shape, up.shape, down.shape,
    ]
    return pl.pallas_call(
        functools.partial(grads_kernel, share, groups),
        out_shape=[jax.ShapeDtypeStruct(o, BF16) for o in outs],
        in_specs=[near if share else far] * 4 + [near] * 6,
        out_specs=[far] * len(outs),
        scratch_shapes=[pltpu.VMEM(o, BF16) for o in outs[1:4]]
        + [pltpu.SemaphoreType.DMA((len(outs),))],
        compiler_params=pltpu.CompilerParams(vmem_limit_bytes=20 * 2**20 if share else VMEM_MOST),
        name="grads",
    )(*arrays)


def on_device(
    client_input,
    client_gain,
    w_query,
    w_keyval,
    w_out,
    server_gain,
    w_gate,
    w_up,
    w_down,
    out_grad,
    valid,
):
    share, results = step_call(
        client_input[0, 0], out_grad[0, 0], valid, client_gain, server_gain,
        w_query[0], w_keyval[0], w_out[0], w_gate[0].T, w_up[0].T, w_down[0],
    )
    (server_out, grad_query, grad_keyval, grad_out, grad_gate, grad_up, grad_down) = grads_call(
        share, w_query.shape[2], *results
    )
    return (
        server_out[None, None],
        grad_query[None],
        grad_keyval[None],
        grad_out[None],
        grad_gate.T[None],
        grad_up.T[None],
        grad_down[None],
    )


def solution(mesh):
    in_specs = (
        P("grp", "mem", None, None),
        P("mem", None),
        P("mem", None, None),
        P("mem", None, None),
        P("mem", None, None),
        P("grp", None),
        P("grp", None, "mem"),
        P("grp", None, "mem"),
        P("grp", "mem", None),
        P("grp", "mem", None, None),
        P("grp", "mem"),
    )
    out_specs = (
        P("grp", "mem", None, None),
        P("mem", None, None),
        P("mem", None, None),
        P("mem", None, None),
        P("grp", None, "mem"),
        P("grp", None, "mem"),
        P("grp", "mem", None),
    )
    return jax.shard_map(
        on_device, mesh=mesh, in_specs=in_specs, out_specs=out_specs, check_vma=False
    )
```

```python
import functools
import math

import jax
import jax.numpy as jnp
from jax import lax
from jax.experimental import pallas as pl
from jax.experimental.pallas import tpu as pltpu
from jax.sharding import PartitionSpec as P

KV_HEADS = 2
HEAD_DIM = 64


EPS = 1e-06
VMEM_MOST = 67043328
F32 = jnp.float32
BF16 = jnp.bfloat16
CONTRACT_LAST = (((1,), (1,)), ((), ()))
CONTRACT_FIRST = (((0,), (0,)), ((), ()))
FIRST_WITH_LAST = (((0,), (1,)), ((), ()))
MESH = pl.DeviceIdType.MESH
SCALE = HEAD_DIM ** (-0.5)


def rms(h_float):
    return lax.rsqrt(jnp.mean(h_float * h_float, axis=-1, keepdims=True) + EPS)


def norm_back(h_float, inv_rms, gain_vec, upstream):
    scaled = upstream * gain_vec
    return inv_rms * scaled - h_float * inv_rms**3 * jnp.mean(
        scaled * h_float, axis=-1, keepdims=True
    )


def dot(left, right, dims=(((1,), (0,)), ((), ()))):
    return lax.dot_general(left, right, dims, preferred_element_type=F32)


class Gather:
    def __init__(self, axis, slot, rows, sems, split=False):
        self.axis, self.slot, self.rows, self.sems = axis, slot, rows, sems
        self.taken = set()
        self.n = lax.axis_size(axis)
        self.pairs = self.n // 2
        me = lax.axis_index(axis)
        self.right = {axis: lax.rem(me + 2, self.n)}
        self.partner = {axis: me + 1 - 2 * lax.rem(me, 2)}
        self.split = split and self.pairs > 1
        self.cut_at = rows // 2

    def send(self, src, dst, first, index, device):
        return pltpu.make_async_remote_copy(
            src_ref=src,
            dst_ref=dst,
            send_sem=self.sems[first].at[index],
            recv_sem=self.sems[first + 1].at[index],
            device_id=device,
            device_id_type=MESH,
        )

    def ring_copy(self, step):
        src, dst = self.slot(2 * step, 0, self.rows), self.slot(2 * step + 2, 0, self.rows)
        return self.send(src, dst, 0, step, self.right)

    def rest_copy(self):
        last, low, count = 2 * self.pairs - 1, self.cut_at, self.rows - self.cut_at
        src, dst = self.slot(last - 2, low, count), self.slot(last, low, count)
        return self.send(src, dst, 0, self.pairs - 1, self.right)

    def flip_copy(self, step):
        rows = self.cut_at if self.split and step == self.pairs - 1 else self.rows
        src, dst = self.slot(2 * step, 0, rows), self.slot(2 * step + 1, 0, rows)
        return self.send(src, dst, 2, step, self.partner)

    def advance(self, step, ring=True):
        if step > 0:
            self.ring_copy(step - 1).wait_recv()
        if ring:
            self.pass_on(step)
        self.flip_copy(step).start()
        if self.split and step == self.pairs - 1:
            self.take(step - 1)
            self.rest_copy().start()

    def pass_on(self, step):
        if step < self.pairs - 1:
            self.ring_copy(step).start()

    def take(self, step):
        if step in self.taken:
            return
        self.taken.add(step)
        self.flip_copy(step).wait_recv()
        if self.split and step == self.pairs - 1:
            self.rest_copy().wait_recv()

    def finish(self):
        for step in range(self.pairs):
            if step < self.pairs - 1:
                self.ring_copy(step).wait_send()
            self.flip_copy(step).wait_send()
        if self.split:
            self.rest_copy().wait_send()


def gather_sems(n):
    return [pltpu.SemaphoreType.DMA((n // 2,))] * 4


def greet(axes):
    barrier = pltpu.get_barrier_semaphore()
    count = 0
    for axis in axes:
        n = lax.axis_size(axis)
        me = lax.axis_index(axis)
        pl.semaphore_signal(
            barrier, 1, device_id={axis: me + 1 - 2 * lax.rem(me, 2)}, device_id_type=MESH
        )
        for k in range(1, n // 2):
            pl.semaphore_signal(
                barrier, 1, device_id={axis: lax.rem(me + 2 * k, n)}, device_id_type=MESH
            )
        count += n // 2
    return lambda: pl.semaphore_wait(barrier, count)


def send(src, dst, sems, index, device):
    return pltpu.make_async_remote_copy(
        src_ref=src,
        dst_ref=dst,
        send_sem=sems[0].at[index],
        recv_sem=sems[1].at[index],
        device_id=device,
        device_id_type=MESH,
    )


def step_kernel(
    share, x_far, og_far, valid, c_gain, s_gain, wq_far, wkv_far, wo_far, gate_far, up_far, down_far,
    server_out, g_gate, g_up, g_down, normed_all, att_all, dqkv_all, cg_all, g_qkv_part, g_out_part,
    x_own, og_own, wq, wkv, wo, gate_w, up_w, down_w,
    q_all, kv_all, p_all,
    cut_slots, rows_cot, rows_normed, hidden, d_gate, d_up,
    served, served_in, home_in, home_out, sums, result, give, give_in, passing, pass_in,
    load_sem, early_sems, late_sems, cut_sems, cot_sems,
    swap_sems, part_sems, home_sems, pass_sems, half_sems,
):
    members, groups = lax.axis_size("mem"), lax.axis_size("grp")
    pairs, group_pairs = members // 2, groups // 2
    length, width = x_own.shape
    half = length // 2
    me = lax.axis_index("mem")
    odd = lax.rem(me, 2)
    partner = {"mem": me + 1 - 2 * odd}
    q_cols = wq.shape[1]
    per_kv = q_cols // HEAD_DIM // KV_HEADS
    kv_rows = KV_HEADS * HEAD_DIM

    loads = {}
    for i, (name, far, near) in enumerate((
        ("x", x_far, x_own), ("og", og_far, og_own), ("wq", wq_far, wq), ("wkv", wkv_far, wkv), ("wo", wo_far, wo),
        ("down", down_far, down_w), ("gate", gate_far, gate_w), ("up", up_far, up_w),
    )):
        loads[name] = pltpu.make_async_copy(far, near, load_sem.at[i])
        loads[name].start()
    met = greet(("grp", "mem"))

    keep_at = pl.multiple_of(odd * half, half)
    give_at = pl.multiple_of((1 - odd) * half, half)

    def half_slot(index, low, count):
        return cg_all.at[index, pl.ds(pl.multiple_of(keep_at + low, 8), count)]

    def whole(ref, base=0):
        return lambda index, low, count: ref.at[index, pl.ds(base + low, count)]

    cut = Gather("mem", whole(cut_slots), length, cut_sems)
    cot_top = Gather("mem", whole(rows_cot), half, cot_sems[0])
    cot_low = Gather("mem", whole(rows_cot, half), half, cot_sems[1])
    early = Gather("grp", whole(normed_all), length, early_sems, True)
    quarter = half // 2
    late_top = Gather("grp", half_slot, quarter, late_sems[0], True)
    late_low = Gather(
        "grp", lambda index, low, count: half_slot(index, quarter + low, count),
        quarter, late_sems[1], True,
    )
    late = (late_top, late_low)

    for name in ("x", "og"):
        loads[name].wait()
    live = lax.broadcasted_iota(jnp.int32, (length, width), 0) < valid[0, 0]
    own_cot = jnp.where(live, og_own[...].astype(F32), 0.0)
    rows_cot[0] = own_cot.astype(BF16)
    sums[...] = own_cot
    x_float = x_own[...].astype(F32)
    normed_all[0] = (x_float * rms(x_float) * c_gain[...]).astype(BF16)
    with jax.named_scope("greet"):
        met()
    cot_top.advance(0)
    cot_low.advance(0, ring=False)
    early.advance(0)

    key_at = lax.broadcasted_iota(jnp.int32, (length, length), 0)
    query_at = lax.broadcasted_iota(jnp.int32, (length, length), 1)
    bias = jnp.where(key_at <= query_at, 0.0, -1e30).astype(F32)
    bias = jnp.concatenate([bias] * per_kv, axis=1)

    def side_by_side(rows, kv):
        first = kv * per_kv * HEAD_DIM
        return jnp.concatenate(
            [rows[first + i * HEAD_DIM : first + (i + 1) * HEAD_DIM] for i in range(per_kv)], axis=1
        )

    def stacked(columns):
        return jnp.concatenate(
            [columns[:, i * length : (i + 1) * length] for i in range(per_kv)], axis=0
        )

    def forward(first, count):
        normed = normed_all[pl.ds(first, count)].reshape(count * length, width)
        queries = (dot(normed, wq[...]) * SCALE).astype(BF16).T
        key_vals = dot(normed, wkv[...]).astype(BF16).T
        for i in range(count):
            slot, span = first + i, slice(i * length, (i + 1) * length)
            kv_all[slot] = key_vals[:, span]
            for kv in range(KV_HEADS):
                keys = key_vals[kv * HEAD_DIM : (kv + 1) * HEAD_DIM, span]
                vals = key_vals[kv_rows + kv * HEAD_DIM : kv_rows + (kv + 1) * HEAD_DIM, span]
                q_cat = side_by_side(queries[:, span], kv)
                q_all[slot, kv] = q_cat
                scores = dot(keys, q_cat, CONTRACT_FIRST) + bias
                expo = jnp.exp(scores - jnp.max(scores, axis=0, keepdims=True))
                probs = (expo * (1.0 / jnp.sum(expo, axis=0, keepdims=True))).astype(BF16)
                p_all[slot, kv] = probs
                att_all[
                    pl.ds(kv * per_kv * HEAD_DIM, per_kv * HEAD_DIM), pl.ds(slot * length, length)
                ] = stacked(dot(vals, probs).astype(BF16))

    def backward(first, count):
        upstream = cg_all[pl.ds(first, count)].reshape(count * length, width)
        d_att = dot(wo[...], upstream, CONTRACT_LAST).astype(BF16)
        for i in range(count):
            slot, span = first + i, slice(i * length, (i + 1) * length)
            columns = pl.ds(slot * length, length)
            for kv in range(KV_HEADS):
                keys = kv_all[slot, pl.ds(kv * HEAD_DIM, HEAD_DIM)]
                vals = kv_all[slot, pl.ds(kv_rows + kv * HEAD_DIM, HEAD_DIM)]
                d_cat = side_by_side(d_att[:, span], kv)
                probs = p_all[slot, kv]
                weighed = dot(vals, d_cat, CONTRACT_FIRST)
                p_float = probs.astype(F32)
                weighed = weighed * p_float
                d_scores = weighed - p_float * jnp.sum(weighed, axis=0, keepdims=True)
                d_scores = d_scores.astype(BF16)
                d_q = (dot(keys, d_scores) * SCALE).astype(BF16)
                dqkv_all[pl.ds(kv * per_kv * HEAD_DIM, per_kv * HEAD_DIM), columns] = stacked(d_q)
                both = dot(
                    jnp.concatenate([q_all[slot, kv], d_cat], axis=0),
                    jnp.concatenate([d_scores, probs], axis=0),
                    CONTRACT_LAST,
                ).astype(BF16)
                dqkv_all[pl.ds(q_cols + kv * HEAD_DIM, HEAD_DIM), columns] = both[:HEAD_DIM, :length]
                dqkv_all[pl.ds(q_cols + kv_rows + kv * HEAD_DIM, HEAD_DIM), columns] = both[
                    HEAD_DIM:, length:
                ]

    with jax.named_scope("wait_wq"):
        loads["wq"].wait()
        loads["wkv"].wait()
    with jax.named_scope("forward_own"):
        forward(0, 1)
    loads["wo"].wait()
    mixed = dot(att_all[:, pl.ds(0, length)], wo[...], CONTRACT_FIRST)
    cut_slots[0] = (x_own[...].astype(F32) + mixed).astype(BF16)
    cut.advance(0)
    cot_low.pass_on(0)

    early_steps = list(range(1, group_pairs))
    done = {"forward": 1, "backward": 0, "partial": 0}

    def keep_going():
        if early_steps:
            step = early_steps.pop(0)
            with jax.named_scope(f"early_step{step}"):
                early.advance(step)

    def recompute(limit):
        while done["forward"] < min(limit, groups):
            first = done["forward"]
            count = 1 if first % 2 else 2
            step = (first + count - 1) // 2
            while early_steps and early_steps[0] <= step:
                keep_going()
            with jax.named_scope(f"early_take{first}"):
                early.take(step)
            with jax.named_scope(f"forward{first}"):
                forward(first, count)
            done["forward"] += count

    def weight_grad(left, right, near):
        rows = right.shape[0] * length
        near[...] = dot(left[...], right[...].reshape(rows, width), CONTRACT_FIRST).astype(BF16)

    weight_grads = [
        (hidden, rows_cot, g_down), (d_gate, rows_normed, g_gate), (d_up, rows_normed, g_up)
    ]

    def more():
        if weight_grads:
            with jax.named_scope(f"weight_grad{len(weight_grads)}"):
                weight_grad(*weight_grads.pop(0))

    def cot_hidden(p):
        with jax.named_scope(f"wait_cot{p}"):
            for part in (cot_top, cot_low):
                if p > 1 or (p == 1 and part is cot_low):
                    part.advance(p)
            for part in (cot_top, cot_low):
                part.take(p)
        left = rows_cot[pl.ds(2 * p, 2)].reshape(2 * length, width)
        return dot(left, down_w[...], CONTRACT_LAST)

    for p in range(pairs):
        span = pl.ds(2 * p, 2)
        if p == 0:
            loads["down"].wait()
            d_hidden = cot_hidden(0)
        with jax.named_scope(f"wait_cut{p}"):
            if p > 0:
                cut.advance(p)
            cut.take(p)
        h_float = cut_slots[span].reshape(2 * length, width).astype(F32)
        inv_rms = rms(h_float)
        normed = (h_float * inv_rms * s_gain[...]).astype(BF16)
        rows_normed[span] = normed.reshape(2, length, width)
        if p == 0:
            for name in ("gate", "up"):
                loads[name].wait()
        gate_act = dot(normed, gate_w[...], CONTRACT_LAST)
        up_act = dot(normed, up_w[...], CONTRACT_LAST)
        if p > 0:
            d_hidden = cot_hidden(p)
        keep_going()
        sigma = jax.nn.sigmoid(gate_act)
        acted = gate_act * sigma
        hidden_now = (acted * up_act).astype(BF16)
        dg = (d_hidden * up_act * sigma * (1.0 + gate_act * (1.0 - sigma))).astype(BF16)
        du = (d_hidden * acted).astype(BF16)
        rows = pl.ds(2 * p * length, 2 * length)
        hidden[rows] = hidden_now
        d_gate[rows] = dg
        d_up[rows] = du
        d_normed = dot(dg, gate_w[...]) + dot(du, up_w[...])
        pushed = norm_back(h_float, inv_rms, s_gain[...], d_normed)
        sums[...] += pushed[:length] + pushed[length:]
        served[span] = dot(hidden_now, down_w[...]).astype(BF16).reshape(2, length, width)
        if p == 0 and pairs > 1:
            with jax.named_scope("cot_step1"):
                cot_top.advance(1)
        if p == 0:
            recompute(2)

    give[...] = sums[pl.ds(give_at, half)].astype(BF16)
    handed = send(give, give_in, part_sems, 0, partner)
    handed.start()
    swaps = []
    for p in range(pairs):
        swaps.append(send(served.at[2 * p + 1], served_in.at[p], swap_sems, p, partner))
        swaps[-1].start()
    with jax.named_scope("wait_handed"):
        handed.wait_recv()
    total = sums[pl.ds(keep_at, half)] + give_in[...].astype(F32)
    passing[...] = total.astype(BF16)
    passes = []
    for k in range(1, pairs):
        passes.append(
            send(passing, pass_in.at[k - 1], pass_sems, k - 1, {"mem": lax.rem(me + 2 * k, members)})
        )
        passes[-1].start()
    recompute(4)
    keep_going()
    homes = []
    for p in range(pairs):
        with jax.named_scope(f"wait_swap{p}"):
            swaps[p].wait_recv()
        mine = served[2 * p].astype(F32) + served_in[p].astype(F32)
        if p == 0:
            result[...] = cut_slots[0].astype(F32) + mine
        else:
            home_out[p - 1] = mine.astype(BF16)
            homes.append(
                send(
                    home_out.at[p - 1], home_in.at[p - 1], home_sems, p - 1,
                    {"mem": lax.rem(me + members - 2 * p, members)},
                )
            )
            homes[-1].start()
    more()
    for k in range(1, pairs):
        with jax.named_scope(f"wait_pass{k}"):
            passes[k - 1].wait_recv()
        total = total + pass_in[k - 1].astype(F32)
    cg_all[0, pl.ds(keep_at, half)] = (total / members).astype(BF16)

    exchanged = {}

    def exchange(slot):
        ref = half_slot(slot, 0, half)
        exchanged[slot] = send(ref, ref, half_sems, slot, partner)
        exchanged[slot].start()

    def partial_grads(count):
        some = pl.ds(0, count * length)
        normed = normed_all[pl.ds(0, count)].reshape(count * length, width)
        g_qkv_part[...] = dot(normed, dqkv_all[:, some], FIRST_WITH_LAST).astype(BF16)
        upstream = cg_all[pl.ds(0, count)].reshape(count * length, width)
        g_out_part[...] = dot(att_all[:, some], upstream).astype(BF16)

    def pull(limit):
        first = done["backward"]
        while first < limit:
            count = min(4, limit - first)
            recompute(first + count)
            for slot in range(first, first + count):
                with jax.named_scope(f"wait_exchange{slot}"):
                    exchanged[slot].wait_recv()
            with jax.named_scope(f"backward{first}"):
                backward(first, count)
            first += count
        done["backward"] = first

    for part in late:
        part.advance(0)
    exchange(0)
    recompute(6)
    more()
    for step in range(1, group_pairs):
        with jax.named_scope(f"late_step{step}"):
            for part in late:
                part.advance(step)
        exchange(2 * step)
        with jax.named_scope(f"late_take{step - 1}"):
            for part in late:
                part.take(step - 1)
        exchange(2 * step - 1)
        if step == 1:
            recompute(8)
            for p in range(1, pairs):
                with jax.named_scope("wait_home"):
                    homes[p - 1].wait_recv()
                result[...] += home_in[p - 1].astype(F32)
            server_out[...] = result[...].astype(BF16)
        elif step % 2 == 0:
            more()
            pull(2 * step)
        if step == group_pairs - 1 and done["backward"] >= share > 0:
            with jax.named_scope("partial"):
                partial_grads(share)
            done["partial"] = share
    while early_steps:
        keep_going()
    recompute(groups)
    while weight_grads:
        more()
    with jax.named_scope("late_last"):
        for part in late:
            part.take(group_pairs - 1)
    exchange(groups - 1)
    pull(groups)
    if not share:
        g_qkv_part[...] = jnp.zeros_like(g_qkv_part)
        g_out_part[...] = jnp.zeros_like(g_out_part)
    elif not done["partial"]:
        partial_grads(share)
    early.finish()
    for part in late:
        part.finish()
    cut.finish()
    cot_top.finish()
    cot_low.finish()
    for copy in [handed] + swaps + passes + homes + list(exchanged.values()):
        copy.wait_send()


def step_call(x, og, valid, c_gain, s_gain, wq, wkv, wo, gate_t, up_t, down):
    members, groups = lax.axis_size("mem"), lax.axis_size("grp")
    pairs = members // 2
    length, width = x.shape
    units = down.shape[0]
    q_cols, kv_cols = wq.shape[1], wkv.shape[1]
    per_kv = q_cols // HEAD_DIM // KV_HEADS
    half = length // 2
    rows = members * length
    tokens = groups * length
    kept = [
        (length, width), (units, width), (units, width), (units, width), (groups, length, width),
        (q_cols, tokens), (q_cols + kv_cols, tokens), (groups, length, width),
        (width, q_cols + kv_cols), (q_cols, width),
    ]
    keep = 2 * sum(math.prod(dims) for dims in kept) < 20 * 2**20
    share = groups // 2 if keep else 0
    if not share:
        kept[-2:] = [(16, 128)] * 2
    shape = lambda *dims: pltpu.VMEM(dims, BF16) if keep else jax.ShapeDtypeStruct(dims, BF16)
    near = pl.BlockSpec(memory_space=pltpu.VMEM)
    far = pl.BlockSpec(memory_space=pl.ANY)
    stay = lambda a: pltpu.with_memory_space_constraint(a, pltpu.HBM)
    others = max(pairs - 1, 1)
    two = lambda count: [pltpu.SemaphoreType.DMA((count,))] * 2
    vmem = lambda *dims: pltpu.VMEM(dims, BF16)
    return share, pl.pallas_call(
        functools.partial(step_kernel, share),
        out_shape=[shape(*dims) for dims in kept],
        in_specs=[far] * 2 + [pl.BlockSpec(memory_space=pltpu.SMEM)] + [near] * 2 + [far] * 6,
        out_specs=[near] * 10,
        scratch_shapes=[
            vmem(length, width), vmem(length, width),
            vmem(*wq.shape), vmem(*wkv.shape), vmem(*wo.shape),
            vmem(units, width), vmem(units, width), vmem(units, width),
            vmem(groups, KV_HEADS, HEAD_DIM, per_kv * length),
            vmem(groups, kv_cols, length),
            vmem(groups, KV_HEADS, length, per_kv * length),
            vmem(members, length, width), vmem(members, length, width), vmem(members, length, width),
            vmem(rows, units), vmem(rows, units), vmem(rows, units),
            vmem(members, length, width),
            vmem(pairs, length, width),
            vmem(others, length, width),
            vmem(others, length, width),
            pltpu.VMEM((length, width), F32),
            pltpu.VMEM((length, width), F32),
            vmem(half, width), vmem(half, width), vmem(half, width),
            vmem(others, half, width),
            pltpu.SemaphoreType.DMA((8,)),
            gather_sems(groups), [gather_sems(groups)] * 2, gather_sems(members), [gather_sems(members)] * 2,
            two(pairs), two(1), two(others), two(others), two(groups),
        ],
        compiler_params=pltpu.CompilerParams(
            collective_id=0, has_side_effects=True, vmem_limit_bytes=38 * 2**20 if keep else VMEM_MOST
        ),
        name="step",
    )(stay(x), stay(og), valid, *map(stay, (c_gain, s_gain, wq, wkv, wo, gate_t, up_t, down)))


def grads_kernel(
    share, groups, server, gate, up, down, normed, att, dqkv, cg, qkv_part, out_part,
    server_out, g_query_out, g_keyval_out, g_out_out, g_gate_out, g_up_out, g_down_out,
    g_query, g_keyval, g_out, store_sem,
):
    tokens = att.shape[1]
    width = normed.shape[2]
    columns = g_query.shape[1]
    stores = []

    def store(near, out):
        stores.append(pltpu.make_async_copy(near, out, store_sem.at[len(stores)]))
        stores[-1].start()

    scale = 1.0 / groups
    for near, out in ((down, g_down_out), (gate, g_gate_out), (up, g_up_out), (server, server_out)):
        store(near, out)
    rest = groups - share
    some = pl.ds(tokens - rest * (tokens // groups), rest * (tokens // groups))
    left = normed[pl.ds(groups - rest, rest)].reshape(-1, width)
    grads = dot(left, dqkv[:, some], FIRST_WITH_LAST)
    if share:
        grads = grads + qkv_part[...].astype(F32)
    grads = grads * scale
    g_query[...] = grads[:, :columns].astype(BF16)
    store(g_query, g_query_out)
    g_keyval[...] = grads[:, columns:].astype(BF16)
    store(g_keyval, g_keyval_out)
    right = cg[pl.ds(groups - rest, rest)].reshape(-1, width)
    grads = dot(att[:, some], right)
    if share:
        grads = grads + out_part[...].astype(F32)
    g_out[...] = (grads * scale).astype(BF16)
    store(g_out, g_out_out)
    for copy in stores:
        copy.wait()


def grads_call(share, columns, *arrays):
    server, gate, up, down, normed, att, dqkv, cg, qkv_part, out_part = arrays
    groups, _, width = normed.shape
    wide = dqkv.shape[0]
    far = pl.BlockSpec(memory_space=pl.ANY)
    near = pl.BlockSpec(memory_space=pltpu.VMEM)
    outs = [
        server.shape, (width, columns), (width, wide - columns), (att.shape[0], width),
        gate.shape, up.shape, down.shape,
    ]
    return pl.pallas_call(
        functools.partial(grads_kernel, share, groups),
        out_shape=[jax.ShapeDtypeStruct(o, BF16) for o in outs],
        in_specs=[near if share else far] * 4 + [near] * 6,
        out_specs=[far] * len(outs),
        scratch_shapes=[pltpu.VMEM(o, BF16) for o in outs[1:4]]
        + [pltpu.SemaphoreType.DMA((len(outs),))],
        compiler_params=pltpu.CompilerParams(vmem_limit_bytes=20 * 2**20 if share else VMEM_MOST),
        name="grads",
    )(*arrays)


def on_device(
    client_input,
    client_gain,
    w_query,
    w_keyval,
    w_out,
    server_gain,
    w_gate,
    w_up,
    w_down,
    out_grad,
    valid,
):
    share, results = step_call(
        client_input[0, 0], out_grad[0, 0], valid, client_gain, server_gain,
        w_query[0], w_keyval[0], w_out[0], w_gate[0].T, w_up[0].T, w_down[0],
    )
    (server_out, grad_query, grad_keyval, grad_out, grad_gate, grad_up, grad_down) = grads_call(
        share, w_query.shape[2], *results
    )
    return (
        server_out[None, None],
        grad_query[None],
        grad_keyval[None],
        grad_out[None],
        grad_gate.T[None],
        grad_up.T[None],
        grad_down[None],
    )


def solution(mesh):
    in_specs = (
        P("grp", "mem", None, None),
        P("mem", None),
        P("mem", None, None),
        P("mem", None, None),
        P("mem", None, None),
        P("grp", None),
        P("grp", None, "mem"),
        P("grp", None, "mem"),
        P("grp", "mem", None),
        P("grp", "mem", None, None),
        P("grp", "mem"),
    )
    out_specs = (
        P("grp", "mem", None, None),
        P("mem", None, None),
        P("mem", None, None),
        P("mem", None, None),
        P("grp", None, "mem"),
        P("grp", None, "mem"),
        P("grp", "mem", None),
    )
    return jax.shard_map(
        on_device, mesh=mesh, in_specs=in_specs, out_specs=out_specs, check_vma=False
    )
```
